256 devices in a mesh: row: 32 (over x, z_lo, y), col: 8 (over z_hi, core).
Axes of the slice: x: 4, y: 4, z: 8 (z_hi: 4, z_lo: 2; z = z_hi * 2 + z_lo), core: 2. Of those that a mesh axis runs over, the one named last changes fastest.
Arguments:
- jacobian: float32 [2, 16384, 256], P(None, ('row', 'col')), may hold values from -0.25 to 0.25
Outputs:
- normal_tiles: float32 [32, 4, 8, 512, 512], P('row', None, 'col')
The draws below stay inside these ranges and needn't reach their ends.
All inputs are finite; a program needn't handle non-finite values.
Results may differ from the reference program's by a relative error of at most 0.0003.
Values sent between devices are 32-bit elements; how exact they have to be, the bound alone decides.
A program may use at most 64 MiB of HBM per device.

```python
import jax
import jax.numpy as jnp
from jax import lax

TILE = 512
KP = 256
PANELS = 2
NT = 32
CYC = 4
M = 16384
N_COL = 8


def block_levels(stream_key, shape, shards, smallest, largest):
    factor_of, own = 1.0, jax.random.fold_in(stream_key, 6)
    for dim, shards_of in shards:
        heights = jnp.exp(jax.random.uniform(jax.random.fold_in(own, dim), (shards_of,), jnp.float32, smallest / len(shards), largest / len(shards)))
        factor_of = factor_of * jnp.repeat(heights, shape[dim] // shards_of).reshape([-1 if axis == dim else 1 for axis in range(len(shape))])
    return factor_of


def gaussian(stream_key, dims, width, limit, pieces=(), kind=jnp.bfloat16):
    result = jax.random.normal(stream_key, dims, jnp.float32) * width
    if len(pieces) > 0:
        result = block_levels(stream_key, dims, pieces, -0.22, 0.18) * result
    return jnp.clip(result, min=-limit, max=limit).astype(kind)


def setup_inputs(seed: int = 0) -> dict:
    streams_of = jax.random.split(jax.random.key(seed), 2)
    jacobian = gaussian(streams_of[0], (PANELS, M, KP), (PANELS * KP) ** -0.5, 0.25, ((1, 256),), jnp.float32)
    return {"jacobian": jacobian}


def reference(jacobian):
    def one_row(index):
        row_block = lax.dynamic_slice_in_dim(jacobian, index * TILE, TILE, 1)
        products = jnp.einsum("pak,pbk->ab", row_block.astype(jnp.float32), jacobian.astype(jnp.float32), precision=lax.Precision.HIGHEST)
        arranged = products.reshape(TILE, CYC, N_COL, TILE).transpose(1, 2, 0, 3)
        column_tile = jnp.arange(CYC, dtype=jnp.int32)[:, None] * N_COL + jnp.arange(N_COL, dtype=jnp.int32)[None, :]
        keep_mask = column_tile <= index
        return jnp.where(keep_mask[:, :, None, None], arranged, jnp.zeros_like(arranged))
    return lax.map(one_row, jnp.arange(NT, dtype=jnp.int32))
```

```python
import jax
import jax.numpy as jnp
from jax import lax
from jax.experimental import pallas as pl
from jax.experimental.pallas import tpu as pltpu
from jax.sharding import PartitionSpec as P

NX, NL, NY, NH, NK = 4, 2, 4, 4, 2
QUARTERS = 4


def class_of(d):
    return ("x" if d in (0, 2) else "y"), (1 if d in (0, 1) else -1)


def hops(d, dt, ds):
    first, way = class_of(d)
    a, b = (dt, ds) if first == "x" else (ds, dt)
    second = "y" if first == "x" else "x"
    if b == 0:
        arrives = None if a == 0 else (first, -way if a == 2 else a)
        sends = []
        if a == 0:
            sends += [(first, 1), (first, -1)]
        elif a == -way:
            sends += [(first, way)]
        sends += [(second, 1), (second, -1)]
    else:
        arrives = (second, -way if b == 2 else b)
        sends = [(second, way)] if b == -way else []
    return arrives, sends


def distance(v):
    return abs(v)


def schedule():
    begin = {0: 0.0, 1: 2.0, 3: 2.0, 2: 4.0}
    order = []
    for d in range(NH):
        for dt in (0, 1, -1, 2):
            for ds in (0, 1, -1, 2):
                steps = distance(dt) + distance(ds)
                order.append((begin[d] + 3.0 * steps, d, dt, ds))
    order.sort(key=lambda e: e[0])
    return order


def mod(v, n):
    return lax.rem(v + 2 * n, n)


def kernel(jac_ref, out_ref, rows, cols, a_cat, b_cat, local_sem, dist_send, dist_recv, row_send, row_recv,
           core_send, core_recv, send_sem, recv_sem):
    row = lax.axis_index("row")
    col = lax.axis_index("col")
    x, l, y = row // 8, (row // 4) % 2, row % 4
    h, k = col // 2, col % 2
    tile = row % 8
    aim_h, aim_k = tile // 2, tile % 2
    from_l, from_y = col // 4, col % 4
    own_column = tile == col

    def device(x_, l_, y_, h_, k_):
        return ((x_ * NL + l_) * NY + y_, h_ * NK + k_)

    def neighbour(axis, way):
        if axis == "x":
            return device(mod(x + way, NX), l, y, h, k)
        if axis == "y":
            return device(x, l, mod(y + way, NY), h, k)
        if axis == "h":
            return device(x, l, y, mod(h + way, NH), k)
        return device(x, l, y, h, 1 - k)

    def remote(src, dst, send, recv, to):
        return pltpu.make_async_remote_copy(
            src_ref=src, dst_ref=dst, send_sem=send, recv_sem=recv, device_id=to,
            device_id_type=pl.DeviceIdType.MESH,
        )

    load = pltpu.make_async_copy(jac_ref, rows.at[col], local_sem.at[0])
    load.start()
    own = pltpu.make_async_copy(jac_ref.at[y], cols.at[x, h, y, k], local_sem.at[1])
    pl.when(own_column)(own.start)

    barrier = pltpu.get_barrier_semaphore()
    greet = [neighbour("x", 1), neighbour("x", -1), neighbour("y", 1), neighbour("y", -1),
             neighbour("h", 1), neighbour("h", -1), neighbour("k", 0)]
    for to in greet:
        pl.semaphore_signal(barrier, inc=1, device_id=to, device_id_type=pl.DeviceIdType.MESH)
    for e in range(NH * NK):
        def signal():
            pl.semaphore_signal(barrier, inc=1, device_id=device(x, from_l, from_y, e // NK, e % NK),
                                device_id_type=pl.DeviceIdType.MESH)
        pl.when((e != col) | jnp.logical_not(own_column))(signal)
    expected = len(greet) + NY * NL
    pl.when(own_column)(lambda: pl.semaphore_wait(barrier, expected - 1))
    pl.when(jnp.logical_not(own_column))(lambda: pl.semaphore_wait(barrier, expected))
    load.wait()

    finish = []

    def go(copy, cond=None):
        if cond is None:
            copy.start()
        else:
            pl.when(cond)(copy.start)
        finish.append((copy, cond))

    for s in range(QUARTERS):
        for l_ in range(NL):
            copy = remote(rows.at[col, s], cols.at[x, h, s, k], dist_send.at[s * NL + l_], dist_recv.at[h, k],
                          device(x, l_, s, aim_h, aim_k))
            mine = own_column & (y == s) & (l == l_)
            go(copy, jnp.logical_not(mine))
    for way in (1, -1):
        n = 0 if way == 1 else 1
        go(remote(rows.at[col], rows.at[col], row_send.at[n], row_recv.at[n], neighbour("h", way)))
    go(remote(rows.at[col], rows.at[col], core_send.at[0], core_recv.at[0], neighbour("k", 0)))

    def rows_arrive(n):
        if n < 2:
            way = 1 if n == 0 else -1
            piece = mod(h - way, NH) * NK + k
            remote(rows.at[piece], rows.at[piece], row_send.at[n], row_recv.at[n], neighbour("h", way)).wait_recv()
            half = rows.at[piece, pl.ds(2 * n, 2)]
            go(remote(half, half, row_send.at[2 + n], row_recv.at[2 + n], neighbour("h", way)))
        else:
            piece = mod(h + 2, NH) * NK + k
            for m in range(2):
                half = rows.at[piece, pl.ds(2 * m, 2)]
                remote(half, half, row_send.at[2 + m], row_recv.at[2 + m], neighbour("h", 1)).wait_recv()
        go(remote(rows.at[piece], rows.at[piece], core_send.at[1 + n], core_recv.at[1 + n], neighbour("k", 0)))

    def cores_arrive():
        for n, dh in enumerate((0, -1, 1, 2)):
            piece = mod(h + dh, NH) * NK + 1 - k
            remote(rows.at[piece], rows.at[piece], core_send.at[n], core_recv.at[n], neighbour("k", 0)).wait_recv()
        for piece in range(NH * NK):
            for s in range(QUARTERS):
                split(rows[piece, s], a_cat, slice(64 * piece + 32 * (s % 2), 64 * piece + 32 * (s % 2) + 32),
                      s // 2, True)

    def split(values, target, at, panel, left):
        high = values.astype(jnp.bfloat16)
        low = (values - high.astype(jnp.float32)).astype(jnp.bfloat16)
        parts = (high, high, low) if left else (high, low, high)
        for n, part in enumerate(parts):
            target[at, 512 * n + 256 * panel : 512 * n + 256 * panel + 256] = part

    counter = [0]

    def there(t, way, plane):
        keeps = plane >= t
        return keeps if way == 1 else keeps | ((t == 1) & (plane == 0))

    def chunk_copy(t, h_, s, n, to):
        chunk = cols.at[t, h_, s]
        return remote(chunk, chunk, send_sem.at[n], recv_sem.at[t, h_, s], to)

    def arrive(d, dt, ds):
        t, h_, s = mod(x + dt, NX), mod(h + d, NH), mod(y + ds, NY)
        first, way = class_of(d)
        came, sends = hops(d, dt, ds)
        here = there(t, way, x)
        passing = None if dt != 0 else True

        def wait():
            if came is None:
                for k_ in range(NK):
                    landed = remote(rows.at[0, 0], cols.at[t, h_, s, k_], dist_send.at[0], dist_recv.at[h_, k_],
                                    neighbour("k", 0))
                    if d == 0:
                        mine = own_column & (k == k_)
                        pl.when(mine)(own.wait)
                        pl.when(jnp.logical_not(mine))(landed.wait_recv)
                    else:
                        landed.wait_recv()
            else:
                chunk_copy(t, h_, s, 0, neighbour("x", 1)).wait_recv()

        if came is None:
            wait()
        elif came[0] == "y":
            if dt == 0:
                wait()
            else:
                pl.when(x > t)(wait)
        else:
            pl.when(here)(wait)
        for axis, step in sends:
            n = counter[0]
            counter[0] += 1
            copy = chunk_copy(t, h_, s, n, neighbour(axis, step))
            if axis == "x":
                go(copy, here & there(t, way, mod(x + step, NX)))
            elif dt == 0:
                go(copy)
            else:
                go(copy, x > t)

    def compute(dt):
        t = mod(x + dt, NX)
        wanted = (t < x) | ((t == x) & (col <= tile))

        def products():
            for h_ in range(NH):
                for s in range(QUARTERS):
                    for k_ in range(NK):
                        at = 128 * h_ + 64 * k_ + 32 * (s % 2)
                        split(cols[t, h_, s, k_], b_cat, slice(at, at + 32), s // 2, False)
            for n in range(2):
                out_ref[0, t, 0, :, 256 * n : 256 * n + 256] = lax.dot_general(
                    a_cat[...], b_cat[256 * n : 256 * n + 256, :], (((1,), (1,)), ((), ())),
                    preferred_element_type=jnp.float32)

        def nothing():
            out_ref[0, t, 0] = jnp.zeros(out_ref.shape[3:], jnp.float32)

        pl.when(wanted)(products)
        pl.when(jnp.logical_not(wanted))(nothing)

    events = [(time, ("chunk", d, dt, ds)) for time, d, dt, ds in schedule()]
    events += [(9.0, ("rows", 0)), (9.0, ("rows", 1)), (12.2, ("rows", 2)), (13.1, ("cores",))]
    events.sort(key=lambda e: e[0])
    for _, event in events:
        if event[0] == "chunk":
            arrive(*event[1:])
        elif event[0] == "rows":
            rows_arrive(event[1])
        else:
            cores_arrive()
    for dt in (0, 1, -1, 2):
        compute(dt)
    for copy, cond in finish:
        if cond is None:
            copy.wait_send()
        else:
            pl.when(cond)(copy.wait_send)


def count_sends():
    return sum(len(hops(d, dt, ds)[1]) for _, d, dt, ds in schedule())


def body(jacobian):
    quarters = jacobian.reshape(QUARTERS, 32, 256)
    dma = pltpu.SemaphoreType.DMA
    return pl.pallas_call(
        kernel,
        out_shape=pltpu.VMEM((1, NX, 1, 512, 512), jnp.float32),
        in_specs=[pl.BlockSpec(memory_space=pltpu.HBM)],
        out_specs=pl.BlockSpec(memory_space=pltpu.VMEM),
        scratch_shapes=[
            pltpu.VMEM((NH * NK, QUARTERS, 32, 256), jnp.float32),
            pltpu.VMEM((NX, NH, QUARTERS, NK, 32, 256), jnp.float32),
            pltpu.VMEM((512, 1536), jnp.bfloat16),
            pltpu.VMEM((512, 1536), jnp.bfloat16),
            dma((2,)),
            dma((QUARTERS * NL,)),
            dma((NH, NK)),
            dma((4,)),
            dma((4,)),
            dma((4,)),
            dma((4,)),
            dma((count_sends(),)),
            dma((NX, NH, QUARTERS)),
        ],
        compiler_params=pltpu.CompilerParams(collective_id=0, has_side_effects=True, vmem_limit_bytes=40 << 20),
    )(quarters)


def solution(mesh):
    return jax.shard_map(
        body, mesh=mesh, in_specs=(P(None, ("row", "col"), None),), out_specs=P("row", None, "col", None, None),
        check_vma=False,
    )
```

```python
import jax
import jax.numpy as jnp
from jax import lax
from jax.experimental import pallas as pl
from jax.experimental.pallas import tpu as pltpu
from jax.sharding import PartitionSpec as P

NX, NL, NY, NH, NK = 4, 2, 4, 4, 2
QUARTERS = 4
VMEM = 62800000


def class_of(d):
    return ("x" if d in (0, 2) else "y"), (1 if d in (0, 1) else -1)


def hops(d, dt, ds):
    first, way = class_of(d)
    a, b = (dt, ds) if first == "x" else (ds, dt)
    second = "y" if first == "x" else "x"
    if b == 0:
        arrives = None if a == 0 else (first, -way if a == 2 else a)
        sends = []
        if a == 0:
            sends += [(first, 1), (first, -1)]
        elif a == -way:
            sends += [(first, way)]
        sends += [(second, 1), (second, -1)]
    else:
        arrives = (second, -way if b == 2 else b)
        sends = [(second, way)] if b == -way else []
    return arrives, sends


ORDER = (
    (0, 0, 0, 0), (0, 1, 0, 0), (0, 3, 0, 0), (0, 0, -1, 0), (0, 2, 0, 0), (0, 1, 0, -1), (0, 3, 0, 1),
    (0, 2, 1, 0), (0, 3, 1, 0), (0, 1, 0, 1), (2, 0), (0, 0, 2, 0), (0, 0, 1, 0), (0, 0, -1, 1), (0, 0, 0, -1),
    (0, 1, -1, -1), (0, 3, 0, -1), (0, 2, -1, 0), (0, 2, 0, 1), (0, 0, 2, 1), (0, 1, 0, 2), (0, 0, -1, -1),
    (0, 3, 0, 2), (0, 1, 1, 1), (0, 0, 0, 1), (0, 0, 1, -1), (0, 0, 2, -1), (0, 1, -1, 1), (0, 3, -1, 0),
    (0, 2, 2, 0), (0, 3, 1, 1), (2, 1), (0, 2, 0, -1), (0, 3, 1, -1), (0, 2, -1, 1), (0, 2, 1, 1), (2, 2),
    (0, 0, 0, 2), (0, 3, -1, -1), (0, 2, 0, 2), (3,), (0, 1, -1, 0), (1, 0, 0), (0, 3, 2, 0), (0, 0, 1, 1),
    (1, 0, 1), (0, 3, -1, 1), (0, 2, 2, 1), (0, 3, 1, 2), (0, 1, -1, 2), (0, 2, -1, -1), (0, 1, 2, 1),
    (0, 1, 1, 0), (0, 1, 1, -1), (0, 0, -1, 2), (0, 1, 2, -1), (1, -1, 0), (0, 0, 1, 2), (0, 2, 1, -1),
    (0, 1, 1, 2), (0, 2, -1, 2), (0, 3, -1, 2), (1, 1, 0), (0, 3, 2, 1), (0, 1, 2, 0), (1, -1, 1), (0, 0, 2, 2),
    (0, 2, 1, 2), (1, 1, 1), (0, 3, 2, -1), (0, 1, 2, 2), (1, 2, 0), (0, 2, 2, -1), (0, 2, 2, 2), (0, 3, 2, 2),
    (1, 2, 1),
)
PAIRS = ((0, 1), (3, 2))


def mod(v, n):
    return lax.rem(v + 2 * n, n)


def kernel(jac_ref, out_ref, rows, cols, a_cat, b_cat, local_sem, dist_send, dist_recv, row_send, row_recv,
           core_send, core_recv, send_sem, recv_sem):
    row = lax.axis_index("row")
    col = lax.axis_index("col")
    x, l, y = row // 8, (row // 4) % 2, row % 4
    h, k = col // 2, col % 2
    tile = row % 8
    aim_h, aim_k = tile // 2, tile % 2
    from_l, from_y = col // 4, col % 4
    own_column = tile == col

    def device(x_, l_, y_, h_, k_):
        return ((x_ * NL + l_) * NY + y_, h_ * NK + k_)

    def neighbour(axis, way):
        if axis == "x":
            return device(mod(x + way, NX), l, y, h, k)
        if axis == "y":
            return device(x, l, mod(y + way, NY), h, k)
        if axis == "h":
            return device(x, l, y, mod(h + way, NH), k)
        return device(x, l, y, h, 1 - k)

    def remote(src, dst, send, recv, to):
        return pltpu.make_async_remote_copy(
            src_ref=src, dst_ref=dst, send_sem=send, recv_sem=recv, device_id=to,
            device_id_type=pl.DeviceIdType.MESH,
        )

    load = pltpu.make_async_copy(jac_ref, rows.at[col], local_sem.at[0])
    load.start()
    own = pltpu.make_async_copy(jac_ref.at[y], cols.at[x, h, y, k], local_sem.at[1])
    pl.when(own_column)(own.start)

    barrier = pltpu.get_barrier_semaphore()
    greet = [neighbour("x", 1), neighbour("x", -1), neighbour("y", 1), neighbour("y", -1),
             neighbour("h", 1), neighbour("h", -1), neighbour("k", 0)]
    for to in greet:
        pl.semaphore_signal(barrier, inc=1, device_id=to, device_id_type=pl.DeviceIdType.MESH)
    for e in range(NH * NK):
        def signal():
            pl.semaphore_signal(barrier, inc=1, device_id=device(x, from_l, from_y, e // NK, e % NK),
                                device_id_type=pl.DeviceIdType.MESH)
        pl.when((e != col) | jnp.logical_not(own_column))(signal)
    def wanted(t):
        return (t < x) | ((t == x) & (col <= tile))

    for t in range(NX):
        def nothing():
            out_ref[0, t, 0] = jnp.zeros(out_ref.shape[3:], jnp.float32)
        pl.when(jnp.logical_not(wanted(t)))(nothing)

    expected = len(greet) + NY * NL
    pl.when(own_column)(lambda: pl.semaphore_wait(barrier, expected - 1))
    pl.when(jnp.logical_not(own_column))(lambda: pl.semaphore_wait(barrier, expected))
    load.wait()

    finish = []

    def go(copy, cond=None):
        if cond is None:
            copy.start()
        else:
            pl.when(cond)(copy.start)
        finish.append((copy, cond))

    for s in range(QUARTERS):
        for l_ in range(NL):
            copy = remote(rows.at[col, s], cols.at[x, h, s, k], dist_send.at[s * NL + l_], dist_recv.at[h, k],
                          device(x, l_, s, aim_h, aim_k))
            mine = own_column & (y == s) & (l == l_)
            go(copy, jnp.logical_not(mine))
    for way in (1, -1):
        n = 0 if way == 1 else 1
        go(remote(rows.at[col], rows.at[col], row_send.at[n], row_recv.at[n], neighbour("h", way)))
    go(remote(rows.at[col], rows.at[col], core_send.at[0], core_recv.at[0], neighbour("k", 0)))

    def rows_arrive(n):
        if n < 2:
            way = 1 if n == 0 else -1
            piece = mod(h - way, NH) * NK + k
            remote(rows.at[piece], rows.at[piece], row_send.at[n], row_recv.at[n], neighbour("h", way)).wait_recv()
            half = rows.at[piece, pl.ds(2 * n, 2)]
            go(remote(half, half, row_send.at[2 + n], row_recv.at[2 + n], neighbour("h", way)))
        else:
            piece = mod(h + 2, NH) * NK + k
            for m in range(2):
                half = rows.at[piece, pl.ds(2 * m, 2)]
                remote(half, half, row_send.at[2 + m], row_recv.at[2 + m], neighbour("h", 1)).wait_recv()
        go(remote(rows.at[piece], rows.at[piece], core_send.at[1 + n], core_recv.at[1 + n], neighbour("k", 0)))

    def cores_arrive():
        for n, dh in enumerate((0, -1, 1, 2)):
            piece = mod(h + dh, NH) * NK + 1 - k
            remote(rows.at[piece], rows.at[piece], core_send.at[n], core_recv.at[n], neighbour("k", 0)).wait_recv()
        for piece in range(NH * NK):
            for s in range(QUARTERS):
                split(rows[piece, s], a_cat, slice(64 * piece + 32 * (s % 2), 64 * piece + 32 * (s % 2) + 32),
                      s // 2, True)

    def split(values, target, at, panel, left):
        high = values.astype(jnp.bfloat16)
        low = (values - high.astype(jnp.float32)).astype(jnp.bfloat16)
        parts = (high, high, low) if left else (high, low, high)
        for n, part in enumerate(parts):
            target[at, 512 * n + 256 * panel : 512 * n + 256 * panel + 256] = part

    counter = [0]

    def there(t, way, plane):
        keeps = plane >= t
        return keeps if way == 1 else keeps | ((t == 1) & (plane == 0))

    def chunk_copy(t, h_, s, n, to):
        chunk = cols.at[t, h_, s]
        return remote(chunk, chunk, send_sem.at[n], recv_sem.at[t, h_, s], to)

    def arrive(d, dt, ds):
        t, h_, s = mod(x + dt, NX), mod(h + d, NH), mod(y + ds, NY)
        first, way = class_of(d)
        came, sends = hops(d, dt, ds)
        here = there(t, way, x)
        passing = None if dt != 0 else True

        def wait():
            if came is None:
                for k_ in range(NK):
                    landed = remote(rows.at[0, 0], cols.at[t, h_, s, k_], dist_send.at[0], dist_recv.at[h_, k_],
                                    neighbour("k", 0))
                    if d == 0:
                        mine = own_column & (k == k_)
                        pl.when(mine)(own.wait)
                        pl.when(jnp.logical_not(mine))(landed.wait_recv)
                    else:
                        landed.wait_recv()
            else:
                chunk_copy(t, h_, s, 0, neighbour("x", 1)).wait_recv()

        if came is None:
            wait()
        elif came[0] == "y":
            if dt == 0:
                wait()
            else:
                pl.when(x > t)(wait)
        else:
            pl.when(here)(wait)
        for axis, step in sends:
            n = counter[0]
            counter[0] += 1
            copy = chunk_copy(t, h_, s, n, neighbour(axis, step))
            if axis == "x":
                go(copy, here & there(t, way, mod(x + step, NX)))
            elif dt == 0:
                go(copy)
            else:
                go(copy, x > t)

    def compute(dt, pair):
        t = mod(x + dt, NX)

        def products():
            for m, d in enumerate(PAIRS[pair]):
                h_ = mod(h + d, NH)
                for s in range(QUARTERS):
                    for k_ in range(NK):
                        at = 128 * m + 64 * k_ + 32 * (s % 2)
                        split(cols[t, h_, s, k_], b_cat, slice(at, at + 32), s // 2, False)
            block = lax.dot_general(
                a_cat[...], b_cat[...], (((1,), (1,)), ((), ())), preferred_element_type=jnp.float32)
            for m, d in enumerate(PAIRS[pair]):
                at = pl.multiple_of(128 * mod(h + d, NH), 128)
                out_ref[0, t, 0, :, pl.ds(at, 128)] = block[:, 128 * m : 128 * m + 128]

        pl.when(wanted(t))(products)

    for event in ORDER:
        if event[0] == 0:
            arrive(*event[1:])
        elif event[0] == 1:
            compute(*event[1:])
        elif event[0] == 2:
            rows_arrive(event[1])
        else:
            cores_arrive()
    for copy, cond in finish:
        if cond is None:
            copy.wait_send()
        else:
            pl.when(cond)(copy.wait_send)


def count_sends():
    return sum(len(hops(*event[1:])[1]) for event in ORDER if event[0] == 0)


def body(jacobian):
    quarters = jacobian.reshape(QUARTERS, 32, 256)
    dma = pltpu.SemaphoreType.DMA
    return pl.pallas_call(
        kernel,
        out_shape=pltpu.VMEM((1, NX, 1, 512, 512), jnp.float32),
        in_specs=[pl.BlockSpec(memory_space=pltpu.HBM)],
        out_specs=pl.BlockSpec(memory_space=pltpu.VMEM),
        scratch_shapes=[
            pltpu.VMEM((NH * NK, QUARTERS, 32, 256), jnp.float32),
            pltpu.VMEM((NX, NH, QUARTERS, NK, 32, 256), jnp.float32),
            pltpu.VMEM((512, 1536), jnp.bfloat16),
            pltpu.VMEM((256, 1536), jnp.bfloat16),
            dma((2,)),
            dma((QUARTERS * NL,)),
            dma((NH, NK)),
            dma((4,)),
            dma((4,)),
            dma((4,)),
            dma((4,)),
            dma((count_sends(),)),
            dma((NX, NH, QUARTERS)),
        ],
        compiler_params=pltpu.CompilerParams(collective_id=0, has_side_effects=True, vmem_limit_bytes=VMEM),
    )(quarters)


def solution(mesh):
    return jax.shard_map(
        body, mesh=mesh, in_specs=(P(None, ("row", "col"), None),), out_specs=P("row", None, "col", None, None),
        check_vma=False,
    )
```

```python
import jax
import jax.numpy as jnp
from jax import lax
from jax.experimental import pallas as pl
from jax.experimental.pallas import tpu as pltpu
from jax.sharding import PartitionSpec as P

NX, NL, NY, NH, NK = 4, 2, 4, 4, 2
QUARTERS = 4
VMEM = 62800000


def class_of(d):
    return ("x" if d in (0, 2) else "y"), (1 if d in (0, 1) else -1)


def hops(d, dt, ds):
    first, way = class_of(d)
    a, b = (dt, ds) if first == "x" else (ds, dt)
    second = "y" if first == "x" else "x"
    if b == 0:
        arrives = None if a == 0 else (first, -way if a == 2 else a)
        sends = []
        if a == 0:
            sends += [(first, 1), (first, -1)]
        elif a == -way:
            sends += [(first, way)]
        sends += [(second, 1), (second, -1)]
    else:
        arrives = (second, -way if b == 2 else b)
        sends = [(second, way)] if b == -way else []
    return arrives, sends


ORDER = (
    (0, 0, 0, 0), (0, 0, 1, 0), (0, 0, -1, 0), (0, 1, 0, 0), (0, 3, 0, 0), (0, 2, 0, 0), (0, 1, 1, 0),
    (0, 0, -1, 1), (2, 0), (0, 1, 0, 1), (0, 0, 0, -1), (2, 1), (0, 3, 0, 1), (0, 1, -1, 0), (0, 3, 0, -1),
    (0, 2, -1, 0), (0, 2, 1, 0), (0, 1, 0, -1), (0, 3, -1, 0), (0, 0, 2, 0), (0, 2, 0, 1), (0, 0, 1, -1),
    (0, 1, -1, 1), (0, 3, 0, 2), (0, 2, -1, 1), (0, 2, 0, -1), (0, 2, 2, 0), (0, 3, 1, 1), (0, 3, 1, 0), (2, 2),
    (0, 2, 1, 1), (0, 0, -1, -1), (0, 3, -1, 1), (0, 0, 0, 1), (0, 2, 1, -1), (0, 0, 0, 2), (0, 3, -1, -1),
    (3,), (0, 3, 1, -1), (0, 2, 0, 2), (0, 0, 1, 1), (0, 2, -1, -1), (0, 1, 0, 2), (0, 0, 2, -1), (0, 2, -1, 2),
    (0, 1, 1, -1), (0, 0, 2, 1), (1, 0, 0), (1, 0, 1), (0, 3, 1, 2), (0, 2, 2, 1), (0, 2, 2, -1), (0, 1, 2, 0),
    (0, 1, -1, -1), (0, 0, 1, 2), (0, 3, -1, 2), (0, 2, 1, 2), (0, 3, 2, 1), (0, 0, -1, 2), (0, 1, 2, 1),
    (1, -1, 1), (0, 1, 1, 1), (0, 1, -1, 2), (0, 3, 2, 0), (0, 1, 2, -1), (1, 1, 1), (1, -1, 0), (0, 1, 1, 2),
    (0, 0, 2, 2), (0, 2, 2, 2), (1, 1, 0), (0, 3, 2, -1), (0, 1, 2, 2), (1, 2, 0), (0, 3, 2, 2), (1, 2, 1),
)
PAIRS = ((0, 1), (3, 2))


def mod(v, n):
    return lax.rem(v + 2 * n, n)


def kernel(jac_ref, out_ref, rows, lines, cols, a_cat, b_cat, local_sem, line_send, line_recv, dist_send, dist_recv,
           row_send, row_recv, core_send, core_recv, send_sem, recv_sem):
    row = lax.axis_index("row")
    col = lax.axis_index("col")
    x, l, y = row // 8, (row // 4) % 2, row % 4
    h, k = col // 2, col % 2
    tile = row % 8
    from_l = col // 4

    def device(x_, l_, y_, h_, k_):
        return ((x_ * NL + l_) * NY + y_, h_ * NK + k_)

    def neighbour(axis, way):
        if axis == "x":
            return device(mod(x + way, NX), l, y, h, k)
        if axis == "y":
            return device(x, l, mod(y + way, NY), h, k)
        if axis == "h":
            return device(x, l, y, mod(h + way, NH), k)
        return device(x, l, y, h, 1 - k)

    def remote(src, dst, send, recv, to):
        return pltpu.make_async_remote_copy(
            src_ref=src, dst_ref=dst, send_sem=send, recv_sem=recv, device_id=to,
            device_id_type=pl.DeviceIdType.MESH,
        )

    load = pltpu.make_async_copy(jac_ref, rows.at[col], local_sem.at[0])
    load.start()
    barrier = pltpu.get_barrier_semaphore()
    greet = [neighbour("x", 1), neighbour("x", -1), neighbour("y", 1), neighbour("y", -1),
             neighbour("y", 2),
             neighbour("h", 1), neighbour("h", -1), neighbour("k", 0)]
    for to in greet:
        pl.semaphore_signal(barrier, inc=1, device_id=to, device_id_type=pl.DeviceIdType.MESH)
    for e in range(NH * NK):
        def signal():
            pl.semaphore_signal(barrier, inc=1, device_id=device(x, from_l, y, e // NK, e % NK),
                                device_id_type=pl.DeviceIdType.MESH)
        pl.when((e != col) | (l != from_l))(signal)
    def wanted(t):
        return (t < x) | ((t == x) & (col <= tile))

    for t in range(NX):
        def nothing():
            out_ref[0, t, 0] = jnp.zeros(out_ref.shape[3:], jnp.float32)
        pl.when(jnp.logical_not(wanted(t)))(nothing)

    expected = len(greet) + NH * NK
    pl.when(l == from_l)(lambda: pl.semaphore_wait(barrier, expected - 1))
    pl.when(l != from_l)(lambda: pl.semaphore_wait(barrier, expected))
    load.wait()

    finish = []

    def go(copy, cond=None):
        if cond is None:
            copy.start()
        else:
            pl.when(cond)(copy.start)
        finish.append((copy, cond))

    def crossing(dy):
        copy = remote(rows.at[col, mod(y + dy, NY)], lines.at[y], line_send.at[dy % NY - 1],
                      line_recv.at[dy % NY - 1], neighbour("y", dy))
        return copy

    for dy in (1, -1, 2):
        go(crossing(dy))
    for dy in (0, 1, -1, 2):
        line = mod(y + dy, NY)
        if dy == 0:
            quarter = rows.at[col, y]
        else:
            quarter = lines.at[line]
            remote(rows.at[col, y], quarter, line_send.at[-dy % NY - 1], line_recv.at[-dy % NY - 1],
                   neighbour("y", dy)).wait_recv()
        aim_h, aim_k = 2 * l + line // 2, line % 2
        for l_ in range(NL):
            to = cols.at[x, h, y, k]
            mine = (aim_h == h) & (aim_k == k) & (l == l_)
            copy = remote(quarter, to, dist_send.at[dy % NY * NL + l_], dist_recv.at[h, k],
                          device(x, l_, y, aim_h, aim_k))
            go(copy, jnp.logical_not(mine))
            stay = pltpu.make_async_copy(quarter, to, local_sem.at[1])
            pl.when(mine)(stay.start)
    for way in (1, -1):
        n = 0 if way == 1 else 1
        go(remote(rows.at[col], rows.at[col], row_send.at[n], row_recv.at[n], neighbour("h", way)))
    go(remote(rows.at[col], rows.at[col], core_send.at[0], core_recv.at[0], neighbour("k", 0)))

    def rows_arrive(n):
        if n < 2:
            way = 1 if n == 0 else -1
            piece = mod(h - way, NH) * NK + k
            remote(rows.at[piece], rows.at[piece], row_send.at[n], row_recv.at[n], neighbour("h", way)).wait_recv()
            half = rows.at[piece, pl.ds(2 * n, 2)]
            go(remote(half, half, row_send.at[2 + n], row_recv.at[2 + n], neighbour("h", way)))
        else:
            piece = mod(h + 2, NH) * NK + k
            for m in range(2):
                half = rows.at[piece, pl.ds(2 * m, 2)]
                remote(half, half, row_send.at[2 + m], row_recv.at[2 + m], neighbour("h", 1)).wait_recv()
        go(remote(rows.at[piece], rows.at[piece], core_send.at[1 + n], core_recv.at[1 + n], neighbour("k", 0)))

    def cores_arrive():
        for n, dh in enumerate((0, -1, 1, 2)):
            piece = mod(h + dh, NH) * NK + 1 - k
            remote(rows.at[piece], rows.at[piece], core_send.at[n], core_recv.at[n], neighbour("k", 0)).wait_recv()
        for piece in range(NH * NK):
            for s in range(QUARTERS):
                split(rows[piece, s], a_cat, slice(64 * piece + 32 * (s % 2), 64 * piece + 32 * (s % 2) + 32),
                      s // 2, True)

    def split(values, target, at, panel, left):
        high = values.astype(jnp.bfloat16)
        low = (values - high.astype(jnp.float32)).astype(jnp.bfloat16)
        parts = (high, high, low) if left else (high, low, high)
        for n, part in enumerate(parts):
            target[at, 512 * n + 256 * panel : 512 * n + 256 * panel + 256] = part

    counter = [0]

    def there(t, way, plane):
        keeps = plane >= t
        return keeps if way == 1 else keeps | ((t == 1) & (plane == 0))

    def chunk_copy(t, h_, s, n, to):
        chunk = cols.at[t, h_, s]
        return remote(chunk, chunk, send_sem.at[n], recv_sem.at[t, h_, s], to)

    def arrive(d, dt, ds):
        t, h_, s = mod(x + dt, NX), mod(h + d, NH), mod(y + ds, NY)
        first, way = class_of(d)
        came, sends = hops(d, dt, ds)
        here = there(t, way, x)
        passing = None if dt != 0 else True

        def wait():
            if came is None:
                for k_ in range(NK):
                    landed = remote(rows.at[0, 0], cols.at[t, h_, s, k_], dist_send.at[0], dist_recv.at[h_, k_],
                                    neighbour("k", 0))
                    if d == 0:
                        mine = (l == from_l) & (k == k_)
                        pl.when(mine)(pltpu.make_async_copy(rows.at[0, 0], cols.at[t, h_, s, k_], local_sem.at[1]).wait)
                        pl.when(jnp.logical_not(mine))(landed.wait_recv)
                    else:
                        landed.wait_recv()
            else:
                chunk_copy(t, h_, s, 0, neighbour("x", 1)).wait_recv()

        if came is None:
            wait()
        elif came[0] == "y":
            if dt == 0:
                wait()
            else:
                pl.when(x > t)(wait)
        else:
            pl.when(here)(wait)
        for axis, step in sends:
            n = counter[0]
            counter[0] += 1
            copy = chunk_copy(t, h_, s, n, neighbour(axis, step))
            if axis == "x":
                go(copy, here & there(t, way, mod(x + step, NX)))
            elif dt == 0:
                go(copy)
            else:
                go(copy, x > t)

    def compute(dt, pair):
        t = mod(x + dt, NX)

        def products():
            for m, d in enumerate(PAIRS[pair]):
                h_ = mod(h + d, NH)
                for s in range(QUARTERS):
                    for k_ in range(NK):
                        at = 128 * m + 64 * k_ + 32 * (s % 2)
                        split(cols[t, h_, s, k_], b_cat, slice(at, at + 32), s // 2, False)
            block = lax.dot_general(
                a_cat[...], b_cat[...], (((1,), (1,)), ((), ())), preferred_element_type=jnp.float32)
            for m, d in enumerate(PAIRS[pair]):
                at = pl.multiple_of(128 * mod(h + d, NH), 128)
                out_ref[0, t, 0, :, pl.ds(at, 128)] = block[:, 128 * m : 128 * m + 128]

        pl.when(wanted(t))(products)

    for event in ORDER:
        if event[0] == 0:
            arrive(*event[1:])
        elif event[0] == 1:
            compute(*event[1:])
        elif event[0] == 2:
            rows_arrive(event[1])
        else:
            cores_arrive()
    for copy, cond in finish:
        if cond is None:
            copy.wait_send()
        else:
            pl.when(cond)(copy.wait_send)


def count_sends():
    return sum(len(hops(*event[1:])[1]) for event in ORDER if event[0] == 0)


def body(jacobian):
    quarters = jacobian.reshape(QUARTERS, 32, 256)
    dma = pltpu.SemaphoreType.DMA
    return pl.pallas_call(
        kernel,
        out_shape=pltpu.VMEM((1, NX, 1, 512, 512), jnp.float32),
        in_specs=[pl.BlockSpec(memory_space=pltpu.HBM)],
        out_specs=pl.BlockSpec(memory_space=pltpu.VMEM),
        scratch_shapes=[
            pltpu.VMEM((NH * NK, QUARTERS, 32, 256), jnp.float32),
            pltpu.VMEM((NY, 32, 256), jnp.float32),
            pltpu.VMEM((NX, NH, QUARTERS, NK, 32, 256), jnp.float32),
            pltpu.VMEM((512, 1536), jnp.bfloat16),
            pltpu.VMEM((256, 1536), jnp.bfloat16),
            dma((2,)),
            dma((NY - 1,)),
            dma((NY - 1,)),
            dma((NY * NL,)),
            dma((NH, NK)),
            dma((4,)),
            dma((4,)),
            dma((4,)),
            dma((4,)),
            dma((count_sends(),)),
            dma((NX, NH, QUARTERS)),
        ],
        compiler_params=pltpu.CompilerParams(collective_id=0, has_side_effects=True, vmem_limit_bytes=VMEM),
    )(quarters)


def solution(mesh):
    return jax.shard_map(
        body, mesh=mesh, in_specs=(P(None, ("row", "col"), None),), out_specs=P("row", None, "col", None, None),
        check_vma=False,
    )
```

```python
import jax
import jax.numpy as jnp
from jax import lax
from jax.experimental import pallas as pl
from jax.experimental.pallas import tpu as pltpu
from jax.sharding import PartitionSpec as P

NX, NL, NY, NH, NK = 4, 2, 4, 4, 2
QUARTERS = 4
VMEM = 56900000


def class_of(d):
    return ("x" if d in (0, 2) else "y"), (1 if d in (0, 1) else -1)


def hops(d, dt, ds):
    first, way = class_of(d)
    a, b = (dt, ds) if first == "x" else (ds, dt)
    second = "y" if first == "x" else "x"
    if b == 0:
        arrives = None if a == 0 else (first, -way if a == 2 else a)
        sends = []
        if a == 0:
            sends += [(first, 1), (first, -1)]
        elif a == -way:
            sends += [(first, way)]
        sends += [(second, 1), (second, -1)]
    else:
        arrives = (second, -way if b == 2 else b)
        sends = [(second, way)] if b == -way else []
    return arrives, sends


ORDER = (
    (0, 0, 0, 0), (0, 0, 1, 0), (0, 0, -1, 0), (0, 1, 0, 0), (0, 3, 0, 0), (0, 2, 0, 0), (0, 1, 1, 0),
    (0, 0, -1, 1), (2, 0), (0, 1, 0, 1), (0, 0, 0, -1), (2, 1), (0, 3, 0, 1), (0, 1, -1, 0), (0, 3, 0, -1),
    (0, 2, -1, 0), (0, 2, 1, 0), (0, 1, 0, -1), (0, 3, -1, 0), (0, 0, 2, 0), (0, 2, 0, 1), (0, 0, 1, -1),
    (0, 1, -1, 1), (0, 3, 0, 2), (0, 2, -1, 1), (0, 2, 0, -1), (0, 2, 2, 0), (0, 3, 1, 1), (0, 3, 1, 0), (2, 2),
    (0, 2, 1, 1), (0, 0, -1, -1), (0, 3, -1, 1), (0, 0, 0, 1), (0, 2, 1, -1), (0, 0, 0, 2), (0, 3, -1, -1),
    (3,), (0, 3, 1, -1), (0, 2, 0, 2), (0, 0, 1, 1), (0, 2, -1, -1), (0, 1, 0, 2), (0, 0, 2, -1), (0, 2, -1, 2),
    (0, 1, 1, -1), (0, 0, 2, 1), (1, 0, 0), (1, 0, 1), (0, 3, 1, 2), (0, 2, 2, 1), (0, 2, 2, -1), (0, 1, 2, 0),
    (0, 1, -1, -1), (0, 0, 1, 2), (0, 3, -1, 2), (0, 2, 1, 2), (0, 3, 2, 1), (0, 0, -1, 2), (0, 1, 2, 1),
    (1, -1, 1), (0, 1, 1, 1), (0, 1, -1, 2), (0, 3, 2, 0), (0, 1, 2, -1), (1, 1, 1), (1, -1, 0), (0, 1, 1, 2),
    (0, 0, 2, 2), (0, 2, 2, 2), (1, 1, 0), (0, 3, 2, -1), (0, 1, 2, 2), (1, 2, 0), (0, 3, 2, 2), (1, 2, 1),
)
PAIRS = ((0, 1), (3, 2))
LATE = tuple(event[1:] for event in ORDER if event[0] == 1)[6:]


def mod(v, n):
    return lax.rem(v + 2 * n, n)


def split(values, target, at, panel, left):
    high = values.astype(jnp.bfloat16)
    low = (values - high.astype(jnp.float32)).astype(jnp.bfloat16)
    parts = (high, high, low) if left else (high, low, high)
    for n, part in enumerate(parts):
        target[at, 512 * n + 256 * panel : 512 * n + 256 * panel + 256] = part


def unit(cols, a_cat, b_cat, t, h, pair):
    for m, d in enumerate(PAIRS[pair]):
        h_ = mod(h + d, NH)
        for s in range(QUARTERS):
            for k_ in range(NK):
                at = 128 * m + 64 * k_ + 32 * (s % 2)
                split(cols[t, h_, s, k_], b_cat, slice(at, at + 32), s // 2, False)
    return lax.dot_general(a_cat[...], b_cat[...], (((1,), (1,)), ((), ())), preferred_element_type=jnp.float32)


def finish_tiles(tiles, a_cat, cols, out_ref, b_cat, late, sem):
    row = lax.axis_index("row")
    col = lax.axis_index("col")
    x, h, tile = row // 8, col // 2, row % 8
    finish = []

    def put(source, dt, d):
        t = mod(x + dt, NX)
        block = pl.ds(pl.multiple_of(128 * mod(h + d, NH), 128), 128)
        source = tiles.at[0, t, 0, :, block] if source is None else source
        return pltpu.make_async_copy(source, out_ref.at[0, t, 0, :, block], sem.at[4 * (dt % NX) + d])

    for dt in (0, 1, -1, 2):
        for pair in range(2):
            t = mod(x + dt, NX)
            waits = ((t < x) | ((t == x) & (col <= tile))) if (dt, pair) in LATE else False
            for d in PAIRS[pair]:
                copy = put(None, dt, d)
                if waits is False:
                    copy.start()
                else:
                    pl.when(jnp.logical_not(waits))(copy.start)
                finish.append(copy)
    for n, (dt, pair) in enumerate(LATE):
        t = mod(x + dt, NX)

        def products():
            block = unit(cols, a_cat, b_cat, t, h, pair)
            for m, d in enumerate(PAIRS[pair]):
                late[2 * n + m] = block[:, 128 * m : 128 * m + 128]
                put(late.at[2 * n + m], dt, d).start()

        pl.when((t < x) | ((t == x) & (col <= tile)))(products)
    for copy in finish:
        copy.wait()


def kernel(jac_ref, out_ref, a_cat, cols, rows, lines, b_cat, local_sem, line_send, line_recv, dist_send, dist_recv,
           row_send, row_recv, core_send, core_recv, send_sem, recv_sem):
    row = lax.axis_index("row")
    col = lax.axis_index("col")
    x, l, y = row // 8, (row // 4) % 2, row % 4
    h, k = col // 2, col % 2
    tile = row % 8
    from_l = col // 4

    def device(x_, l_, y_, h_, k_):
        return ((x_ * NL + l_) * NY + y_, h_ * NK + k_)

    def neighbour(axis, way):
        if axis == "x":
            return device(mod(x + way, NX), l, y, h, k)
        if axis == "y":
            return device(x, l, mod(y + way, NY), h, k)
        if axis == "h":
            return device(x, l, y, mod(h + way, NH), k)
        return device(x, l, y, h, 1 - k)

    def remote(src, dst, send, recv, to):
        return pltpu.make_async_remote_copy(
            src_ref=src, dst_ref=dst, send_sem=send, recv_sem=recv, device_id=to,
            device_id_type=pl.DeviceIdType.MESH,
        )

    load = pltpu.make_async_copy(jac_ref, rows.at[col], local_sem.at[0])
    load.start()
    barrier = pltpu.get_barrier_semaphore()
    greet = [neighbour("x", 1), neighbour("x", -1), neighbour("y", 1), neighbour("y", -1),
             neighbour("y", 2),
             neighbour("h", 1), neighbour("h", -1), neighbour("k", 0)]
    for to in greet:
        pl.semaphore_signal(barrier, inc=1, device_id=to, device_id_type=pl.DeviceIdType.MESH)
    for e in range(NH * NK):
        def signal():
            pl.semaphore_signal(barrier, inc=1, device_id=device(x, from_l, y, e // NK, e % NK),
                                device_id_type=pl.DeviceIdType.MESH)
        pl.when((e != col) | (l != from_l))(signal)
    def wanted(t):
        return (t < x) | ((t == x) & (col <= tile))

    for t in range(NX):
        def nothing():
            out_ref[0, t, 0] = jnp.zeros(out_ref.shape[3:], jnp.float32)
        pl.when(jnp.logical_not(wanted(t)))(nothing)

    expected = len(greet) + NH * NK
    pl.when(l == from_l)(lambda: pl.semaphore_wait(barrier, expected - 1))
    pl.when(l != from_l)(lambda: pl.semaphore_wait(barrier, expected))
    load.wait()

    finish = []

    def go(copy, cond=None):
        if cond is None:
            copy.start()
        else:
            pl.when(cond)(copy.start)
        finish.append((copy, cond))

    def crossing(dy):
        copy = remote(rows.at[col, mod(y + dy, NY)], lines.at[y], line_send.at[dy % NY - 1],
                      line_recv.at[dy % NY - 1], neighbour("y", dy))
        return copy

    for dy in (1, -1, 2):
        go(crossing(dy))
    for dy in (0, 1, -1, 2):
        line = mod(y + dy, NY)
        if dy == 0:
            quarter = rows.at[col, y]
        else:
            quarter = lines.at[line]
            remote(rows.at[col, y], quarter, line_send.at[-dy % NY - 1], line_recv.at[-dy % NY - 1],
                   neighbour("y", dy)).wait_recv()
        aim_h, aim_k = 2 * l + line // 2, line % 2
        for l_ in range(NL):
            to = cols.at[x, h, y, k]
            mine = (aim_h == h) & (aim_k == k) & (l == l_)
            copy = remote(quarter, to, dist_send.at[dy % NY * NL + l_], dist_recv.at[h, k],
                          device(x, l_, y, aim_h, aim_k))
            go(copy, jnp.logical_not(mine))
            stay = pltpu.make_async_copy(quarter, to, local_sem.at[1])
            pl.when(mine)(stay.start)
    for way in (1, -1):
        n = 0 if way == 1 else 1
        go(remote(rows.at[col], rows.at[col], row_send.at[n], row_recv.at[n], neighbour("h", way)))
    go(remote(rows.at[col], rows.at[col], core_send.at[0], core_recv.at[0], neighbour("k", 0)))

    def rows_arrive(n):
        if n < 2:
            way = 1 if n == 0 else -1
            piece = mod(h - way, NH) * NK + k
            remote(rows.at[piece], rows.at[piece], row_send.at[n], row_recv.at[n], neighbour("h", way)).wait_recv()
            half = rows.at[piece, pl.ds(2 * n, 2)]
            go(remote(half, half, row_send.at[2 + n], row_recv.at[2 + n], neighbour("h", way)))
        else:
            piece = mod(h + 2, NH) * NK + k
            for m in range(2):
                half = rows.at[piece, pl.ds(2 * m, 2)]
                remote(half, half, row_send.at[2 + m], row_recv.at[2 + m], neighbour("h", 1)).wait_recv()
        go(remote(rows.at[piece], rows.at[piece], core_send.at[1 + n], core_recv.at[1 + n], neighbour("k", 0)))

    def cores_arrive():
        for n, dh in enumerate((0, -1, 1, 2)):
            piece = mod(h + dh, NH) * NK + 1 - k
            remote(rows.at[piece], rows.at[piece], core_send.at[n], core_recv.at[n], neighbour("k", 0)).wait_recv()
        for piece in range(NH * NK):
            for s in range(QUARTERS):
                split(rows[piece, s], a_cat, slice(64 * piece + 32 * (s % 2), 64 * piece + 32 * (s % 2) + 32),
                      s // 2, True)

    counter = [0]

    def there(t, way, plane):
        keeps = plane >= t
        return keeps if way == 1 else keeps | ((t == 1) & (plane == 0))

    def chunk_copy(t, h_, s, n, to):
        chunk = cols.at[t, h_, s]
        return remote(chunk, chunk, send_sem.at[n], recv_sem.at[t, h_, s], to)

    def arrive(d, dt, ds):
        t, h_, s = mod(x + dt, NX), mod(h + d, NH), mod(y + ds, NY)
        first, way = class_of(d)
        came, sends = hops(d, dt, ds)
        here = there(t, way, x)
        passing = None if dt != 0 else True

        def wait():
            if came is None:
                for k_ in range(NK):
                    landed = remote(rows.at[0, 0], cols.at[t, h_, s, k_], dist_send.at[0], dist_recv.at[h_, k_],
                                    neighbour("k", 0))
                    if d == 0:
                        mine = (l == from_l) & (k == k_)
                        pl.when(mine)(pltpu.make_async_copy(rows.at[0, 0], cols.at[t, h_, s, k_], local_sem.at[1]).wait)
                        pl.when(jnp.logical_not(mine))(landed.wait_recv)
                    else:
                        landed.wait_recv()
            else:
                chunk_copy(t, h_, s, 0, neighbour("x", 1)).wait_recv()

        if came is None:
            wait()
        elif came[0] == "y":
            if dt == 0:
                wait()
            else:
                pl.when(x > t)(wait)
        else:
            pl.when(here)(wait)
        for axis, step in sends:
            n = counter[0]
            counter[0] += 1
            copy = chunk_copy(t, h_, s, n, neighbour(axis, step))
            if axis == "x":
                go(copy, here & there(t, way, mod(x + step, NX)))
            elif dt == 0:
                go(copy)
            else:
                go(copy, x > t)

    def compute(dt, pair):
        t = mod(x + dt, NX)

        def products():
            block = unit(cols, a_cat, b_cat, t, h, pair)
            for m, d in enumerate(PAIRS[pair]):
                at = pl.multiple_of(128 * mod(h + d, NH), 128)
                out_ref[0, t, 0, :, pl.ds(at, 128)] = block[:, 128 * m : 128 * m + 128]

        pl.when(wanted(t))(products)

    for event in ORDER:
        if event[0] == 0:
            arrive(*event[1:])
        elif event[0] == 1:
            if event[1:] not in LATE:
                compute(*event[1:])
        elif event[0] == 2:
            rows_arrive(event[1])
        else:
            cores_arrive()
    for copy, cond in finish:
        if cond is None:
            copy.wait_send()
        else:
            pl.when(cond)(copy.wait_send)


def count_sends():
    return sum(len(hops(*event[1:])[1]) for event in ORDER if event[0] == 0)


def body(jacobian):
    quarters = jacobian.reshape(QUARTERS, 32, 256)
    dma = pltpu.SemaphoreType.DMA
    tiles, rows_cat, cols = pl.pallas_call(
        kernel,
        out_shape=(
            pltpu.VMEM((1, NX, 1, 512, 512), jnp.float32),
            pltpu.VMEM((512, 1536), jnp.bfloat16),
            pltpu.VMEM((NX, NH, QUARTERS, NK, 32, 256), jnp.float32),
        ),
        in_specs=[pl.BlockSpec(memory_space=pltpu.HBM)],
        out_specs=(pl.BlockSpec(memory_space=pltpu.VMEM),) * 3,
        scratch_shapes=[
            pltpu.VMEM((NH * NK, QUARTERS, 32, 256), jnp.float32),
            pltpu.VMEM((NY, 32, 256), jnp.float32),
            pltpu.VMEM((256, 1536), jnp.bfloat16),
            dma((2,)),
            dma((NY - 1,)),
            dma((NY - 1,)),
            dma((NY * NL,)),
            dma((NH, NK)),
            dma((4,)),
            dma((4,)),
            dma((4,)),
            dma((4,)),
            dma((count_sends(),)),
            dma((NX, NH, QUARTERS)),
        ],
        compiler_params=pltpu.CompilerParams(collective_id=0, has_side_effects=True, vmem_limit_bytes=VMEM),
    )(quarters)
    return pl.pallas_call(
        finish_tiles,
        out_shape=jax.ShapeDtypeStruct((1, NX, 1, 512, 512), jnp.float32),
        in_specs=[pl.BlockSpec(memory_space=pltpu.VMEM)] * 3,
        out_specs=pl.BlockSpec(memory_space=pltpu.HBM),
        scratch_shapes=[
            pltpu.VMEM((256, 1536), jnp.bfloat16),
            pltpu.VMEM((max(1, 2 * len(LATE)), 512, 128), jnp.float32),
            dma((4 * NX,)),
        ],
        compiler_params=pltpu.CompilerParams(vmem_limit_bytes=8 << 20),
    )(tiles, rows_cat, cols)


def solution(mesh):
    return jax.shard_map(
        body, mesh=mesh, in_specs=(P(None, ("row", "col"), None),), out_specs=P("row", None, "col", None, None),
        check_vma=False,
    )
```

```python
import jax
import jax.numpy as jnp
from jax import lax
from jax.experimental import pallas as pl
from jax.experimental.pallas import tpu as pltpu
from jax.sharding import PartitionSpec as P

NX, NL, NY, NH, NK = 4, 2, 4, 4, 2
QUARTERS = 4
VMEM = 56900000


def class_of(d):
    return ("x" if d in (0, 2) else "y"), (1 if d in (0, 1) else -1)


def hops(d, dt, ds):
    first, way = class_of(d)
    a, b = (dt, ds) if first == "x" else (ds, dt)
    second = "y" if first == "x" else "x"
    if b == 0:
        arrives = None if a == 0 else (first, -way if a == 2 else a)
        sends = []
        if a == 0:
            sends += [(first, 1), (first, -1)]
        elif a == -way:
            sends += [(first, way)]
        sends += [(second, 1), (second, -1)]
    else:
        arrives = (second, -way if b == 2 else b)
        sends = [(second, way)] if b == -way else []
    return arrives, sends


ORDER = (
    (0, 0, 0, 0), (0, 0, 1, 0), (0, 0, -1, 0), (0, 1, 0, 0), (0, 3, 0, 0), (0, 2, 0, 0), (0, 1, 1, 0),
    (0, 0, -1, 1), (2, 0), (0, 1, 0, 1), (0, 0, 0, -1), (2, 1), (0, 3, 0, 1), (0, 1, -1, 0), (0, 3, 0, -1),
    (0, 2, -1, 0), (0, 2, 1, 0), (0, 1, 0, -1), (0, 3, -1, 0), (0, 0, 2, 0), (0, 2, 0, 1), (0, 0, 1, -1),
    (0, 1, -1, 1), (0, 3, 0, 2), (0, 2, -1, 1), (0, 2, 0, -1), (0, 2, 2, 0), (0, 3, 1, 1), (0, 3, 1, 0), (2, 2),
    (0, 2, 1, 1), (0, 0, -1, -1), (0, 3, -1, 1), (0, 0, 0, 1), (3,), (0, 2, 1, -1), (0, 0, 0, 2),
    (0, 3, -1, -1), (0, 3, 1, -1), (0, 2, 0, 2), (0, 0, 1, 1), (0, 2, -1, -1), (0, 1, 0, 2), (0, 0, 2, -1),
    (0, 2, -1, 2), (0, 1, 1, -1), (0, 0, 2, 1), (1, 0, 0), (1, 0, 1), (0, 3, 1, 2), (0, 2, 2, 1), (0, 2, 2, -1),
    (0, 1, 2, 0), (0, 1, -1, -1), (0, 0, 1, 2), (0, 3, -1, 2), (0, 2, 1, 2), (0, 3, 2, 1), (0, 0, -1, 2),
    (0, 1, 2, 1), (1, -1, 1), (0, 1, 1, 1), (0, 1, -1, 2), (0, 3, 2, 0), (0, 1, 2, -1), (1, 1, 1), (1, -1, 0),
    (0, 1, 1, 2), (0, 0, 2, 2), (0, 2, 2, 2), (1, 1, 0), (0, 3, 2, -1), (0, 1, 2, 2), (1, 2, 0), (0, 3, 2, 2),
    (1, 2, 1),
)
PAIRS = ((0, 1), (3, 2))
LATE = tuple(event[1:] for event in ORDER if event[0] == 1)[6:]


def mod(v, n):
    return lax.rem(v + 2 * n, n)


def split(values, target, at, panel, left):
    high = values.astype(jnp.bfloat16)
    low = (values - high.astype(jnp.float32)).astype(jnp.bfloat16)
    parts = (high, high, low) if left else (high, low, high)
    for n, part in enumerate(parts):
        target[at, 512 * n + 256 * panel : 512 * n + 256 * panel + 256] = part


def unit(cols, a_cat, b_cat, t, h, pair):
    for m, d in enumerate(PAIRS[pair]):
        h_ = mod(h + d, NH)
        for s in range(QUARTERS):
            for k_ in range(NK):
                at = 128 * m + 64 * k_ + 32 * (s % 2)
                split(cols[t, h_, s, k_], b_cat, slice(at, at + 32), s // 2, False)
    return lax.dot_general(a_cat[...], b_cat[...], (((1,), (1,)), ((), ())), preferred_element_type=jnp.float32)


def finish_tiles(tiles, a_cat, cols, out_ref, b_cat, late, sem):
    row = lax.axis_index("row")
    col = lax.axis_index("col")
    x, h, tile = row // 8, col // 2, row % 8
    finish = []

    def put(source, dt, d):
        t = mod(x + dt, NX)
        block = pl.ds(pl.multiple_of(128 * mod(h + d, NH), 128), 128)
        source = tiles.at[0, t, 0, :, block] if source is None else source
        return pltpu.make_async_copy(source, out_ref.at[0, t, 0, :, block], sem.at[4 * (dt % NX) + d])

    for dt in (0, 1, -1, 2):
        for pair in range(2):
            t = mod(x + dt, NX)
            waits = ((t < x) | ((t == x) & (col <= tile))) if (dt, pair) in LATE else False
            for d in PAIRS[pair]:
                copy = put(None, dt, d)
                if waits is False:
                    copy.start()
                else:
                    pl.when(jnp.logical_not(waits))(copy.start)
                finish.append(copy)
    for n, (dt, pair) in enumerate(LATE):
        t = mod(x + dt, NX)

        def products():
            block = unit(cols, a_cat, b_cat, t, h, pair)
            for m, d in enumerate(PAIRS[pair]):
                late[2 * n + m] = block[:, 128 * m : 128 * m + 128]
                put(late.at[2 * n + m], dt, d).start()

        pl.when((t < x) | ((t == x) & (col <= tile)))(products)
    for copy in finish:
        copy.wait()


def kernel(jac_ref, out_ref, a_cat, cols, rows, lines, b_cat, local_sem, line_send, line_recv, dist_send, dist_recv,
           row_send, row_recv, core_send, core_recv, send_sem, recv_sem):
    row = lax.axis_index("row")
    col = lax.axis_index("col")
    x, l, y = row // 8, (row // 4) % 2, row % 4
    h, k = col // 2, col % 2
    tile = row % 8
    from_l = col // 4

    def device(x_, l_, y_, h_, k_):
        return ((x_ * NL + l_) * NY + y_, h_ * NK + k_)

    def neighbour(axis, way):
        if axis == "x":
            return device(mod(x + way, NX), l, y, h, k)
        if axis == "y":
            return device(x, l, mod(y + way, NY), h, k)
        if axis == "h":
            return device(x, l, y, mod(h + way, NH), k)
        return device(x, l, y, h, 1 - k)

    def remote(src, dst, send, recv, to):
        return pltpu.make_async_remote_copy(
            src_ref=src, dst_ref=dst, send_sem=send, recv_sem=recv, device_id=to,
            device_id_type=pl.DeviceIdType.MESH,
        )

    load = pltpu.make_async_copy(jac_ref, rows.at[col], local_sem.at[0])
    load.start()
    barrier = pltpu.get_barrier_semaphore()
    greet = [neighbour("x", 1), neighbour("x", -1), neighbour("y", 1), neighbour("y", -1),
             neighbour("y", 2),
             neighbour("h", 1), neighbour("h", -1), neighbour("k", 0)]
    for to in greet:
        pl.semaphore_signal(barrier, inc=1, device_id=to, device_id_type=pl.DeviceIdType.MESH)
    for e in range(NH * NK):
        def signal():
            pl.semaphore_signal(barrier, inc=1, device_id=device(x, from_l, y, e // NK, e % NK),
                                device_id_type=pl.DeviceIdType.MESH)
        pl.when((e != col) | (l != from_l))(signal)
    def wanted(t):
        return (t < x) | ((t == x) & (col <= tile))

    for t in range(NX):
        def nothing():
            out_ref[0, t, 0] = jnp.zeros(out_ref.shape[3:], jnp.float32)
        pl.when(jnp.logical_not(wanted(t)))(nothing)

    expected = len(greet) + NH * NK
    pl.when(l == from_l)(lambda: pl.semaphore_wait(barrier, expected - 1))
    pl.when(l != from_l)(lambda: pl.semaphore_wait(barrier, expected))
    load.wait()

    finish = []

    def go(copy, cond=None):
        if cond is None:
            copy.start()
        else:
            pl.when(cond)(copy.start)
        finish.append((copy, cond))

    def crossing(dy):
        copy = remote(rows.at[col, mod(y + dy, NY)], lines.at[y], line_send.at[dy % NY - 1],
                      line_recv.at[dy % NY - 1], neighbour("y", dy))
        return copy

    for dy in (1, -1, 2):
        go(crossing(dy))
    for dy in (0, 1, -1, 2):
        line = mod(y + dy, NY)
        if dy == 0:
            quarter = rows.at[col, y]
        else:
            quarter = lines.at[line]
            remote(rows.at[col, y], quarter, line_send.at[-dy % NY - 1], line_recv.at[-dy % NY - 1],
                   neighbour("y", dy)).wait_recv()
        aim_h, aim_k = 2 * l + line // 2, line % 2
        for l_ in range(NL):
            to = cols.at[x, h, y, k]
            mine = (aim_h == h) & (aim_k == k) & (l == l_)
            copy = remote(quarter, to, dist_send.at[dy % NY * NL + l_], dist_recv.at[h, k],
                          device(x, l_, y, aim_h, aim_k))
            go(copy, jnp.logical_not(mine))
            stay = pltpu.make_async_copy(quarter, to, local_sem.at[1])
            pl.when(mine)(stay.start)
    for way in (1, -1):
        n = 0 if way == 1 else 1
        go(remote(rows.at[col], rows.at[col], row_send.at[n], row_recv.at[n], neighbour("h", way)))
    go(remote(rows.at[col], rows.at[col], core_send.at[0], core_recv.at[0], neighbour("k", 0)))

    def rows_arrive(n):
        if n < 2:
            way = 1 if n == 0 else -1
            piece = mod(h - way, NH) * NK + k
            remote(rows.at[piece], rows.at[piece], row_send.at[n], row_recv.at[n], neighbour("h", way)).wait_recv()
            half = rows.at[piece, pl.ds(2 * n, 2)]
            go(remote(half, half, row_send.at[2 + n], row_recv.at[2 + n], neighbour("h", way)))
        else:
            piece = mod(h + 2, NH) * NK + k
            for m in range(2):
                half = rows.at[piece, pl.ds(2 * m, 2)]
                remote(half, half, row_send.at[2 + m], row_recv.at[2 + m], neighbour("h", 1)).wait_recv()
        go(remote(rows.at[piece], rows.at[piece], core_send.at[1 + n], core_recv.at[1 + n], neighbour("k", 0)))

    def cores_arrive():
        for n, dh in enumerate((0, -1, 1, 2)):
            piece = mod(h + dh, NH) * NK + 1 - k
            remote(rows.at[piece], rows.at[piece], core_send.at[n], core_recv.at[n], neighbour("k", 0)).wait_recv()
        for piece in range(NH * NK):
            for s in range(QUARTERS):
                split(rows[piece, s], a_cat, slice(64 * piece + 32 * (s % 2), 64 * piece + 32 * (s % 2) + 32),
                      s // 2, True)

    counter = [0]

    def there(t, way, plane):
        keeps = plane >= t
        return keeps if way == 1 else keeps | ((t == 1) & (plane == 0))

    def chunk_copy(t, h_, s, n, to):
        chunk = cols.at[t, h_, s]
        return remote(chunk, chunk, send_sem.at[n], recv_sem.at[t, h_, s], to)

    def arrive(d, dt, ds):
        t, h_, s = mod(x + dt, NX), mod(h + d, NH), mod(y + ds, NY)
        first, way = class_of(d)
        came, sends = hops(d, dt, ds)
        here = there(t, way, x)
        passing = None if dt != 0 else True

        def wait():
            if came is None:
                for k_ in range(NK):
                    landed = remote(rows.at[0, 0], cols.at[t, h_, s, k_], dist_send.at[0], dist_recv.at[h_, k_],
                                    neighbour("k", 0))
                    if d == 0:
                        mine = (l == from_l) & (k == k_)
                        pl.when(mine)(pltpu.make_async_copy(rows.at[0, 0], cols.at[t, h_, s, k_], local_sem.at[1]).wait)
                        pl.when(jnp.logical_not(mine))(landed.wait_recv)
                    else:
                        landed.wait_recv()
            else:
                chunk_copy(t, h_, s, 0, neighbour("x", 1)).wait_recv()

        if came is None:
            wait()
        elif came[0] == "y":
            if dt == 0:
                wait()
            else:
                pl.when(x > t)(wait)
        else:
            pl.when(here)(wait)
        for axis, step in sends:
            n = counter[0]
            counter[0] += 1
            copy = chunk_copy(t, h_, s, n, neighbour(axis, step))
            if axis == "x":
                go(copy, here & there(t, way, mod(x + step, NX)))
            elif dt == 0:
                go(copy)
            else:
                go(copy, x > t)

    def compute(dt, pair):
        t = mod(x + dt, NX)

        def products():
            block = unit(cols, a_cat, b_cat, t, h, pair)
            for m, d in enumerate(PAIRS[pair]):
                at = pl.multiple_of(128 * mod(h + d, NH), 128)
                out_ref[0, t, 0, :, pl.ds(at, 128)] = block[:, 128 * m : 128 * m + 128]

        pl.when(wanted(t))(products)

    for event in ORDER:
        if event[0] == 0:
            arrive(*event[1:])
        elif event[0] == 1:
            if event[1:] not in LATE:
                compute(*event[1:])
        elif event[0] == 2:
            rows_arrive(event[1])
        else:
            cores_arrive()
    for copy, cond in finish:
        if cond is None:
            copy.wait_send()
        else:
            pl.when(cond)(copy.wait_send)


def count_sends():
    return sum(len(hops(*event[1:])[1]) for event in ORDER if event[0] == 0)


def body(jacobian):
    quarters = jacobian.reshape(QUARTERS, 32, 256)
    dma = pltpu.SemaphoreType.DMA
    tiles, rows_cat, cols = pl.pallas_call(
        kernel,
        out_shape=(
            pltpu.VMEM((1, NX, 1, 512, 512), jnp.float32),
            pltpu.VMEM((512, 1536), jnp.bfloat16),
            pltpu.VMEM((NX, NH, QUARTERS, NK, 32, 256), jnp.float32),
        ),
        in_specs=[pl.BlockSpec(memory_space=pltpu.HBM)],
        out_specs=(pl.BlockSpec(memory_space=pltpu.VMEM),) * 3,
        scratch_shapes=[
            pltpu.VMEM((NH * NK, QUARTERS, 32, 256), jnp.float32),
            pltpu.VMEM((NY, 32, 256), jnp.float32),
            pltpu.VMEM((256, 1536), jnp.bfloat16),
            dma((2,)),
            dma((NY - 1,)),
            dma((NY - 1,)),
            dma((NY * NL,)),
            dma((NH, NK)),
            dma((4,)),
            dma((4,)),
            dma((4,)),
            dma((4,)),
            dma((count_sends(),)),
            dma((NX, NH, QUARTERS)),
        ],
        compiler_params=pltpu.CompilerParams(collective_id=0, has_side_effects=True, vmem_limit_bytes=VMEM),
    )(quarters)
    return pl.pallas_call(
        finish_tiles,
        out_shape=jax.ShapeDtypeStruct((1, NX, 1, 512, 512), jnp.float32),
        in_specs=[pl.BlockSpec(memory_space=pltpu.VMEM)] * 3,
        out_specs=pl.BlockSpec(memory_space=pltpu.HBM),
        scratch_shapes=[
            pltpu.VMEM((256, 1536), jnp.bfloat16),
            pltpu.VMEM((max(1, 2 * len(LATE)), 512, 128), jnp.float32),
            dma((4 * NX,)),
        ],
        compiler_params=pltpu.CompilerParams(vmem_limit_bytes=8 << 20),
    )(tiles, rows_cat, cols)


def solution(mesh):
    return jax.shard_map(
        body, mesh=mesh, in_specs=(P(None, ("row", "col"), None),), out_specs=P("row", None, "col", None, None),
        check_vma=False,
    )
```

```python
import jax
import jax.numpy as jnp
from jax import lax
from jax.experimental import pallas as pl
from jax.experimental.pallas import tpu as pltpu
from jax.sharding import PartitionSpec as P

NX, NL, NY, NH, NK = 4, 2, 4, 4, 2
QUARTERS = 4
VMEM = 56900000


def class_of(d):
    return ("x" if d in (0, 2) else "y"), (1 if d in (0, 1) else -1)


def hops(d, dt, ds):
    first, way = class_of(d)
    a, b = (dt, ds) if first == "x" else (ds, dt)
    second = "y" if first == "x" else "x"
    if b == 0:
        arrives = None if a == 0 else (first, -way if a == 2 else a)
        sends = []
        if a == 0:
            sends += [(first, 1), (first, -1)]
        elif a == -way:
            sends += [(first, way)]
        sends += [(second, 1), (second, -1)]
    else:
        arrives = (second, -way if b == 2 else b)
        sends = [(second, way)] if b == -way else []
    return arrives, sends


ORDER = (
    (0, 0, 0, 0), (0, 0, 1, 0), (0, 0, -1, 0), (0, 1, 0, 0), (0, 3, 0, 0), (0, 2, 0, 0), (0, 1, 1, 0),
    (0, 0, -1, 1), (2, 0), (0, 1, 0, 1), (0, 0, 0, -1), (2, 1), (0, 3, 0, 1), (0, 1, -1, 0), (0, 3, 0, -1),
    (0, 2, -1, 0), (0, 2, 1, 0), (0, 1, 0, -1), (0, 3, -1, 0), (0, 0, 2, 0), (0, 2, 0, 1), (0, 0, 1, -1),
    (0, 1, -1, 1), (0, 3, 0, 2), (0, 2, -1, 1), (0, 2, 0, -1), (0, 2, 2, 0), (0, 3, 1, 1), (0, 3, 1, 0), (2, 2),
    (0, 2, 1, 1), (0, 0, -1, -1), (0, 3, -1, 1), (0, 0, 0, 1), (3,), (0, 2, 1, -1), (0, 0, 0, 2),
    (0, 3, -1, -1), (0, 3, 1, -1), (0, 2, 0, 2), (0, 0, 1, 1), (0, 2, -1, -1), (0, 1, 0, 2), (0, 0, 2, -1),
    (0, 2, -1, 2), (0, 1, 1, -1), (0, 0, 2, 1), (1, 0, 0), (1, 0, 1), (0, 3, 1, 2), (0, 2, 2, 1), (0, 2, 2, -1),
    (0, 1, 2, 0), (0, 1, -1, -1), (0, 0, 1, 2), (0, 3, -1, 2), (0, 2, 1, 2), (0, 3, 2, 1), (0, 0, -1, 2),
    (0, 1, 2, 1), (1, -1, 1), (0, 1, 1, 1), (0, 1, -1, 2), (0, 3, 2, 0), (0, 1, 2, -1), (1, 1, 1), (1, -1, 0),
    (0, 1, 1, 2), (0, 0, 2, 2), (0, 2, 2, 2), (1, 1, 0), (0, 3, 2, -1), (0, 1, 2, 2), (1, 2, 0), (0, 3, 2, 2),
    (1, 2, 1),
)
PAIRS = ((0, 1), (3, 2))
LATE = tuple(event[1:] for event in ORDER if event[0] == 1)[6:]


def mod(v, n):
    return lax.rem(v + 2 * n, n)


def split(values, target, at, panel, left):
    high = values.astype(jnp.bfloat16)
    low = (values - high.astype(jnp.float32)).astype(jnp.bfloat16)
    parts = (high, high, low) if left else (high, low, high)
    for n, part in enumerate(parts):
        target[at, 512 * n + 256 * panel : 512 * n + 256 * panel + 256] = part


def unit(cols, a_cat, b_cat, t, h, pair):
    for m, d in enumerate(PAIRS[pair]):
        h_ = mod(h + d, NH)
        for s in range(QUARTERS):
            for k_ in range(NK):
                at = 128 * m + 64 * k_ + 32 * (s % 2)
                split(cols[t, h_, s, k_], b_cat, slice(at, at + 32), s // 2, False)
    return lax.dot_general(a_cat[...], b_cat[...], (((1,), (1,)), ((), ())), preferred_element_type=jnp.float32)


def finish_tiles(tiles, a_cat, cols, out_ref, b_cat, late, sem):
    row = lax.axis_index("row")
    col = lax.axis_index("col")
    x, h, tile = row // 8, col // 2, row % 8
    finish = []

    def put(source, dt, d):
        t = mod(x + dt, NX)
        block = pl.ds(pl.multiple_of(128 * mod(h + d, NH), 128), 128)
        source = tiles.at[0, t, 0, :, block] if source is None else source
        return pltpu.make_async_copy(source, out_ref.at[0, t, 0, :, block], sem.at[4 * (dt % NX) + d])

    for dt in (0, 1, -1, 2):
        for pair in range(2):
            t = mod(x + dt, NX)
            waits = ((t < x) | ((t == x) & (col <= tile))) if (dt, pair) in LATE else False
            for d in PAIRS[pair]:
                copy = put(None, dt, d)
                if waits is False:
                    copy.start()
                else:
                    pl.when(jnp.logical_not(waits))(copy.start)
                finish.append(copy)
    for n, (dt, pair) in enumerate(LATE):
        t = mod(x + dt, NX)

        def products():
            block = unit(cols, a_cat, b_cat, t, h, pair)
            for m, d in enumerate(PAIRS[pair]):
                late[2 * n + m] = block[:, 128 * m : 128 * m + 128]
                put(late.at[2 * n + m], dt, d).start()

        pl.when((t < x) | ((t == x) & (col <= tile)))(products)
    for copy in finish:
        copy.wait()


def kernel(jac_ref, out_ref, a_cat, cols, rows, lines, b_cat, local_sem, line_send, line_recv, dist_send, dist_recv,
           row_send, row_recv, core_send, core_recv, send_sem, recv_sem):
    row = lax.axis_index("row")
    col = lax.axis_index("col")
    x, l, y = row // 8, (row // 4) % 2, row % 4
    h, k = col // 2, col % 2
    tile = row % 8
    from_l = col // 4

    def device(x_, l_, y_, h_, k_):
        return ((x_ * NL + l_) * NY + y_, h_ * NK + k_)

    def neighbour(axis, way):
        if axis == "x":
            return device(mod(x + way, NX), l, y, h, k)
        if axis == "y":
            return device(x, l, mod(y + way, NY), h, k)
        if axis == "h":
            return device(x, l, y, mod(h + way, NH), k)
        return device(x, l, y, h, 1 - k)

    def remote(src, dst, send, recv, to):
        return pltpu.make_async_remote_copy(
            src_ref=src, dst_ref=dst, send_sem=send, recv_sem=recv, device_id=to,
            device_id_type=pl.DeviceIdType.MESH,
        )

    load = pltpu.make_async_copy(jac_ref, rows.at[col], local_sem.at[0])
    load.start()
    barrier = pltpu.get_barrier_semaphore()
    greet = [neighbour("x", 1), neighbour("x", -1), neighbour("y", 1), neighbour("y", -1),
             neighbour("y", 2),
             neighbour("h", 1), neighbour("h", -1), neighbour("k", 0)]
    for to in greet:
        pl.semaphore_signal(barrier, inc=1, device_id=to, device_id_type=pl.DeviceIdType.MESH)
    for e in range(NH * NK):
        def signal():
            pl.semaphore_signal(barrier, inc=1, device_id=device(x, from_l, y, e // NK, e % NK),
                                device_id_type=pl.DeviceIdType.MESH)
        pl.when((e != col) | (l != from_l))(signal)
    def wanted(t):
        return (t < x) | ((t == x) & (col <= tile))

    for t in range(NX):
        def nothing():
            out_ref[0, t, 0] = jnp.zeros(out_ref.shape[3:], jnp.float32)
        pl.when(jnp.logical_not(wanted(t)))(nothing)

    expected = len(greet) + NH * NK
    pl.when(l == from_l)(lambda: pl.semaphore_wait(barrier, expected - 1))
    pl.when(l != from_l)(lambda: pl.semaphore_wait(barrier, expected))
    load.wait()

    finish = []

    def go(copy, cond=None):
        if cond is None:
            copy.start()
        else:
            pl.when(cond)(copy.start)
        finish.append((copy, cond))

    def crossing(dy):
        copy = remote(rows.at[col, mod(y + dy, NY)], lines.at[y], line_send.at[dy % NY - 1],
                      line_recv.at[dy % NY - 1], neighbour("y", dy))
        return copy

    for dy in (2, 1, -1):
        go(crossing(dy))
    for dy in (0, 1, -1, 2):
        line = mod(y + dy, NY)
        if dy == 0:
            quarter = rows.at[col, y]
        else:
            quarter = lines.at[line]
            remote(rows.at[col, y], quarter, line_send.at[-dy % NY - 1], line_recv.at[-dy % NY - 1],
                   neighbour("y", dy)).wait_recv()
        aim_h, aim_k = 2 * l + line // 2, line % 2
        for l_ in range(NL):
            to = cols.at[x, h, y, k]
            mine = (aim_h == h) & (aim_k == k) & (l == l_)
            copy = remote(quarter, to, dist_send.at[dy % NY * NL + l_], dist_recv.at[h, k],
                          device(x, l_, y, aim_h, aim_k))
            go(copy, jnp.logical_not(mine))
            stay = pltpu.make_async_copy(quarter, to, local_sem.at[1])
            pl.when(mine)(stay.start)
    for way in (1, -1):
        n = 0 if way == 1 else 1
        go(remote(rows.at[col], rows.at[col], row_send.at[n], row_recv.at[n], neighbour("h", way)))
    go(remote(rows.at[col], rows.at[col], core_send.at[0], core_recv.at[0], neighbour("k", 0)))

    def rows_arrive(n):
        if n < 2:
            way = 1 if n == 0 else -1
            piece = mod(h - way, NH) * NK + k
            remote(rows.at[piece], rows.at[piece], row_send.at[n], row_recv.at[n], neighbour("h", way)).wait_recv()
            half = rows.at[piece, pl.ds(2 * n, 2)]
            go(remote(half, half, row_send.at[2 + n], row_recv.at[2 + n], neighbour("h", way)))
        else:
            piece = mod(h + 2, NH) * NK + k
            for m in range(2):
                half = rows.at[piece, pl.ds(2 * m, 2)]
                remote(half, half, row_send.at[2 + m], row_recv.at[2 + m], neighbour("h", 1)).wait_recv()
        go(remote(rows.at[piece], rows.at[piece], core_send.at[1 + n], core_recv.at[1 + n], neighbour("k", 0)))

    def cores_arrive():
        for n, dh in enumerate((0, -1, 1, 2)):
            piece = mod(h + dh, NH) * NK + 1 - k
            remote(rows.at[piece], rows.at[piece], core_send.at[n], core_recv.at[n], neighbour("k", 0)).wait_recv()
        for piece in range(NH * NK):
            for s in range(QUARTERS):
                split(rows[piece, s], a_cat, slice(64 * piece + 32 * (s % 2), 64 * piece + 32 * (s % 2) + 32),
                      s // 2, True)

    counter = [0]

    def there(t, way, plane):
        keeps = plane >= t
        return keeps if way == 1 else keeps | ((t == 1) & (plane == 0))

    def chunk_copy(t, h_, s, n, to):
        chunk = cols.at[t, h_, s]
        return remote(chunk, chunk, send_sem.at[n], recv_sem.at[t, h_, s], to)

    def arrive(d, dt, ds):
        t, h_, s = mod(x + dt, NX), mod(h + d, NH), mod(y + ds, NY)
        first, way = class_of(d)
        came, sends = hops(d, dt, ds)
        here = there(t, way, x)
        passing = None if dt != 0 else True

        def wait():
            if came is None:
                for k_ in range(NK):
                    landed = remote(rows.at[0, 0], cols.at[t, h_, s, k_], dist_send.at[0], dist_recv.at[h_, k_],
                                    neighbour("k", 0))
                    if d == 0:
                        mine = (l == from_l) & (k == k_)
                        pl.when(mine)(pltpu.make_async_copy(rows.at[0, 0], cols.at[t, h_, s, k_], local_sem.at[1]).wait)
                        pl.when(jnp.logical_not(mine))(landed.wait_recv)
                    else:
                        landed.wait_recv()
            else:
                chunk_copy(t, h_, s, 0, neighbour("x", 1)).wait_recv()

        if came is None:
            wait()
        elif came[0] == "y":
            if dt == 0:
                wait()
            else:
                pl.when(x > t)(wait)
        else:
            pl.when(here)(wait)
        for axis, step in sends:
            n = counter[0]
            counter[0] += 1
            copy = chunk_copy(t, h_, s, n, neighbour(axis, step))
            if axis == "x":
                go(copy, here & there(t, way, mod(x + step, NX)))
            elif dt == 0:
                go(copy)
            else:
                go(copy, x > t)

    def compute(dt, pair):
        t = mod(x + dt, NX)

        def products():
            block = unit(cols, a_cat, b_cat, t, h, pair)
            for m, d in enumerate(PAIRS[pair]):
                at = pl.multiple_of(128 * mod(h + d, NH), 128)
                out_ref[0, t, 0, :, pl.ds(at, 128)] = block[:, 128 * m : 128 * m + 128]

        pl.when(wanted(t))(products)

    for event in ORDER:
        if event[0] == 0:
            arrive(*event[1:])
        elif event[0] == 1:
            if event[1:] not in LATE:
                compute(*event[1:])
        elif event[0] == 2:
            rows_arrive(event[1])
        else:
            cores_arrive()
    for copy, cond in finish:
        if cond is None:
            copy.wait_send()
        else:
            pl.when(cond)(copy.wait_send)


def count_sends():
    return sum(len(hops(*event[1:])[1]) for event in ORDER if event[0] == 0)


def body(jacobian):
    quarters = jacobian.reshape(QUARTERS, 32, 256)
    dma = pltpu.SemaphoreType.DMA
    tiles, rows_cat, cols = pl.pallas_call(
        kernel,
        out_shape=(
            pltpu.VMEM((1, NX, 1, 512, 512), jnp.float32),
            pltpu.VMEM((512, 1536), jnp.bfloat16),
            pltpu.VMEM((NX, NH, QUARTERS, NK, 32, 256), jnp.float32),
        ),
        in_specs=[pl.BlockSpec(memory_space=pltpu.HBM)],
        out_specs=(pl.BlockSpec(memory_space=pltpu.VMEM),) * 3,
        scratch_shapes=[
            pltpu.VMEM((NH * NK, QUARTERS, 32, 256), jnp.float32),
            pltpu.VMEM((NY, 32, 256), jnp.float32),
            pltpu.VMEM((256, 1536), jnp.bfloat16),
            dma((2,)),
            dma((NY - 1,)),
            dma((NY - 1,)),
            dma((NY * NL,)),
            dma((NH, NK)),
            dma((4,)),
            dma((4,)),
            dma((4,)),
            dma((4,)),
            dma((count_sends(),)),
            dma((NX, NH, QUARTERS)),
        ],
        compiler_params=pltpu.CompilerParams(collective_id=0, has_side_effects=True, vmem_limit_bytes=VMEM),
    )(quarters)
    return pl.pallas_call(
        finish_tiles,
        out_shape=jax.ShapeDtypeStruct((1, NX, 1, 512, 512), jnp.float32),
        in_specs=[pl.BlockSpec(memory_space=pltpu.VMEM)] * 3,
        out_specs=pl.BlockSpec(memory_space=pltpu.HBM),
        scratch_shapes=[
            pltpu.VMEM((256, 1536), jnp.bfloat16),
            pltpu.VMEM((max(1, 2 * len(LATE)), 512, 128), jnp.float32),
            dma((4 * NX,)),
        ],
        compiler_params=pltpu.CompilerParams(vmem_limit_bytes=8 << 20),
    )(tiles, rows_cat, cols)


def solution(mesh):
    return jax.shard_map(
        body, mesh=mesh, in_specs=(P(None, ("row", "col"), None),), out_specs=P("row", None, "col", None, None),
        check_vma=False,
    )
```
